32 devices in a mesh: replica: 16 (over z, x, core), shard: 2 (over y).
Axes of the slice: x: 2, y: 2, z: 4, core: 2. Of those that a mesh axis runs over, the one named last changes fastest.
Arguments:
- tokens: bfloat16 [16, 2, 512, 768], P('replica', None, 'shard'), may hold values from -6 to 6
- cotangent: bfloat16 [16, 2, 512, 768], P('replica', None, 'shard'), may hold values from -6 to 6
- seq_units: int32 [16, 2], P('replica'), may hold values from 0 to 2, as said below
- deal: int32 [16, 2], P('replica'), may hold values from 0 to 1, as said below
- timesteps: int32 [16, 2], P('replica'), may hold values from 0 to 999
- ln_gain: bfloat16 [768], P('shard'), may hold values from 0.5 to 1.5
- ln_bias: bfloat16 [768], P('shard'), may hold values from -2 to 2
- qkv_weight: bfloat16 [768, 2304], P('shard'), may hold values from -0.21875 to 0.21875
- qkv_bias: bfloat16 [2304], P('shard'), may hold values from -2 to 2
- out_weight: bfloat16 [768, 768], P('shard'), may hold values from -2.5 to 2.5
- out_bias: bfloat16 [768], P('shard'), may hold values from -2 to 2
- ada_weight: bfloat16 [128, 2304], P('shard'), may hold values from -0.5 to 0.5
- ada_bias: bfloat16 [2304], P('shard'), may hold values from -3 to 3
- up_weight: bfloat16 [768, 3072], P('shard'), may hold values from -0.21875 to 0.21875
- up_bias: bfloat16 [3072], P('shard'), may hold values from -2 to 2
- down_weight: bfloat16 [3072, 768], P('shard'), may hold values from -0.109375 to 0.109375
- down_bias: bfloat16 [768], P('shard'), may hold values from -2 to 2
Outputs:
- mixed: bfloat16 [16, 2, 512, 768], P('replica', None, 'shard')
- held: bfloat16 [16, 2, 1024, 768], P('replica', 'shard')
- grad_tokens: bfloat16 [16, 2, 512, 768], P('replica', None, 'shard')
- grad_ln_gain: float32 [768], P('shard')
- grad_ln_bias: float32 [768], P('shard')
- grad_qkv_weight: float32 [768, 2304], P('shard')
- grad_qkv_bias: float32 [2304], P('shard')
- grad_out_weight: float32 [768, 768], P('shard')
- grad_out_bias: float32 [768], P('shard')
- grad_ada_weight: float32 [128, 2304], P('shard')
- grad_ada_bias: float32 [2304], P('shard')
- grad_up_weight: float32 [768, 3072], P('shard')
- grad_up_bias: float32 [3072], P('shard')
- grad_down_weight: float32 [3072, 768], P('shard')
- grad_down_bias: float32 [768], P('shard')
The draws below stay inside these ranges and needn't reach their ends.
Inputs may be any that keep to these rules, and one draw needn't show every extreme that they name: `seq_units`: each row lists the group's sequences in the order in which they lie; an entry is 1 or 2 units for a used sequence and 0 for an unused one, and unused entries may stand anywhere in the row; a row sums to 2, and at least one sequence of every row has 2 units. Each row is a permutation of the 2 owners of a group; sequence j goes to owner deal[g, j], and owners named by unused entries receive nothing, so an owner receives at most one sequence. `timesteps`: entries of unused sequences are not read.
All inputs are finite; a program needn't handle non-finite values.
Results may differ from the reference program's by a relative error of at most 0.019.
Values may be sent and summed in bfloat16 or wider, within the bound.
A program may use at most 192 MiB of HBM per device.

```python
import math
import jax
import jax.numpy as jnp
from jax import lax

D = 768
HEADS = 12
HD = 64
FF = 3072
TDIM = 128
TSTEPS = 1000
TOK_DEV = 512
UNITS = 2
GROUPS = 16


def layout_draw(key):
    base = jax.random.fold_in(key, 17)

    def one_group(subkey):
        first_key, second_key, third_key = jax.random.split(subkey, 3)
        doubles = jax.random.randint(first_key, (), 1, UNITS // 2 + 1)
        count = UNITS - doubles
        slots = jnp.arange(UNITS, dtype=jnp.int32)
        scores = jax.random.randint(second_key, (UNITS,), 0, 1 << 20) * UNITS + slots
        order = jnp.argsort(scores, stable=True)
        template = jnp.where(slots < doubles, 2, jnp.where(slots < count, 1, 0)).astype(jnp.int32)
        units = jnp.zeros((UNITS,), jnp.int32).at[order].set(template)
        dealt = jax.random.permutation(third_key, UNITS).astype(jnp.int32)
        return (units, dealt)
    return jax.vmap(one_group)(jax.random.split(base, GROUPS))


def draw_seq_units(key, part):
    return layout_draw(key)[0]


def draw_deal(key, part):
    return layout_draw(key)[1]


def set_ends(values, stream_key, low, high):
    longest = values.shape.index(max(values.shape))
    spots = []
    for shift in (0, 1):
        where = [jax.random.randint(jax.random.fold_in(stream_key, axis), (), 0, length) for axis, length in enumerate(values.shape)]
        where[longest] = (where[longest] + shift) % values.shape[longest]
        spots.append(tuple(where))
    return values.at[spots[0]].set(low).at[spots[1]].set(high)


def steps_of(rng, shape, cuts, least, high):
    def one(axis_at, shards_of):
        steps = jax.random.uniform(jax.random.fold_in(jax.random.fold_in(rng, 6), axis_at), (shards_of,), jnp.float32, least / len(cuts), high / len(cuts))
        return jnp.repeat(jnp.exp(steps), shape[axis_at] // shards_of).reshape((-1,) + (1,) * (len(shape) - axis_at - 1))

    loudness = one(*cuts[0])
    for cut in cuts[1:]:
        loudness = loudness * one(*cut)
    return loudness


def scatter_about(rng, shape, scale, most, shards=(), held_as=jnp.bfloat16):
    level = steps_of(rng, shape, shards, -0.22, 0.18) if shards else 1.0
    entries = jax.random.normal(rng, shape, jnp.float32) * scale * level
    return jnp.minimum(jnp.maximum(entries, -most), most).astype(held_as)


def setup_inputs(seed: int = 0) -> dict:
    key_of = jax.random.split(jax.random.key(seed), 18)
    tokens = scatter_about(key_of[0], (GROUPS, UNITS, TOK_DEV, D), 1.0, 6.0, ((0, 16), (2, 2)))
    cotangent = scatter_about(key_of[1], (GROUPS, UNITS, TOK_DEV, D), 1.0, 6.0, ((0, 16), (2, 2)))
    seq_units = draw_seq_units(jax.random.fold_in(key_of[17], 71), 0)
    deal = draw_deal(jax.random.fold_in(key_of[17], 71), 0)
    timesteps = set_ends(jax.random.randint(key_of[4], (GROUPS, UNITS), 0, TSTEPS), jax.random.fold_in(key_of[4], 1), 0, TSTEPS - 1).astype(jnp.int32)
    ln_gain = jnp.clip(1.0 + 0.1 * jax.random.normal(key_of[5], (D,), jnp.float32), 0.5, 1.5).astype(jnp.bfloat16)
    ln_bias = scatter_about(key_of[6], (D,), 0.3, 2.0, ((0, 2),))
    qkv_weight = scatter_about(key_of[7], (D, 3 * D), D ** -0.5, 0.21875, ((0, 2),))
    qkv_bias = scatter_about(key_of[8], (3 * D,), 0.3, 2.0, ((0, 2),))
    out_weight = scatter_about(key_of[9], (D, D), (max(4 * D // TOK_DEV, 1)) ** -0.5, 2.5, ((0, 2),))
    out_bias = scatter_about(key_of[10], (D,), 0.3, 2.0, ((0, 2),))
    ada_weight = scatter_about(key_of[11], (TDIM, 3 * D), TDIM ** -0.5, 0.5, ((0, 2),))
    ada_bias = scatter_about(key_of[12], (3 * D,), 0.5, 3.0, ((0, 2),))
    up_weight = scatter_about(key_of[13], (D, FF), D ** -0.5, 0.21875, ((0, 2),))
    up_bias = scatter_about(key_of[14], (FF,), 0.3, 2.0, ((0, 2),))
    down_weight = scatter_about(key_of[15], (FF, D), FF ** -0.5, 0.109375, ((0, 2),))
    down_bias = scatter_about(key_of[16], (D,), 0.3, 2.0, ((0, 2),))
    return dict(tokens=tokens, cotangent=cotangent, seq_units=seq_units, deal=deal, timesteps=timesteps, ln_gain=ln_gain, ln_bias=ln_bias, qkv_weight=qkv_weight, qkv_bias=qkv_bias, out_weight=out_weight, out_bias=out_bias, ada_weight=ada_weight, ada_bias=ada_bias, up_weight=up_weight, up_bias=up_bias, down_weight=down_weight, down_bias=down_bias)


@jax.custom_vjp
def low(v):
    return lax.optimization_barrier(v.astype(jnp.bfloat16)).astype(jnp.float32)

@jax.custom_vjp
def low_back(v):
    return v

def low_keep(v):
    return (low(v), None)

def low_pass(kept, grad):
    return (grad,)

def back_keep(v):
    return (v, None)

def back_low(kept, grad):
    return (low(grad),)
low.defvjp(low_keep, low_pass)
low_back.defvjp(back_keep, back_low)
EPSILON = 1e-05
NEGATIVE = -1000000000.0
HIGHEST = lax.Precision.HIGHEST

def matmul_high(left, right):
    return jnp.dot(left, right, precision=HIGHEST, preferred_element_type=jnp.float32)

def layer_norm(values):
    center = values - lax.optimization_barrier(jnp.mean(values, axis=-1, keepdims=True))
    spread = lax.optimization_barrier(jnp.mean(center * center, axis=-1, keepdims=True))
    return center * lax.rsqrt(spread + EPSILON)

def rotary_tables(length, head_dim):
    half = head_dim // 2
    freqs = jnp.exp(-math.log(10000.0) * jnp.arange(half, dtype=jnp.float32) / half)
    angles = jnp.arange(length, dtype=jnp.float32)[:, None] * freqs[None, :]
    return (jnp.cos(angles)[:, None, :], jnp.sin(angles)[:, None, :])

def rotate(field, cosines, sines):
    half = field.shape[-1] // 2
    first = field[..., :half]
    second = field[..., half:]
    return jnp.concatenate([first * cosines - second * sines, second * cosines + first * sines], axis=-1)

def time_features(step, width):
    half = width // 2
    freqs = jnp.exp(-math.log(10000.0) * jnp.arange(half, dtype=jnp.float32) / half)
    angles = step.astype(jnp.float32) * freqs
    return jnp.concatenate([jnp.cos(angles), jnp.sin(angles)])

def sequence_forward(params, rows, count, step):
    gain, shift_bias, qkv_weight, qkv_bias, out_weight, out_bias, ada_weight, ada_bias, up_weight, up_bias, down_weight, down_bias = params
    length = rows.shape[0]
    key_live = jnp.arange(length, dtype=jnp.int32) < count * TOK_DEV
    normed_in = low(layer_norm(rows) * gain + shift_bias)
    projected = low_back(matmul_high(normed_in, qkv_weight) + qkv_bias)
    cosines, sines = rotary_tables(length, HD)
    queries = low(rotate(projected[:, :D].reshape(length, HEADS, HD), cosines, sines))
    key_rows = low(rotate(projected[:, D:2 * D].reshape(length, HEADS, HD), cosines, sines))
    value_rows = low(projected[:, 2 * D:].reshape(length, HEADS, HD))
    factor = 1.0 / math.sqrt(HD)

    def one_head(items):
        query_head, key_head, value_head = items
        scores = low_back(matmul_high(query_head, key_head.T) * factor)
        scores = jnp.where(key_live[None, :], scores, NEGATIVE)
        highest = lax.optimization_barrier(jnp.max(scores, axis=1, keepdims=True))
        expon = jnp.exp(scores - highest)
        probs = expon / lax.optimization_barrier(jnp.sum(expon, axis=1, keepdims=True))
        return matmul_high(low(probs), value_head)
    heads_out = lax.map(jax.checkpoint(one_head), (queries.transpose(1, 0, 2), key_rows.transpose(1, 0, 2), value_rows.transpose(1, 0, 2)))
    attended = low(low_back(heads_out.transpose(1, 0, 2).reshape(length, D)))
    branch = low_back(matmul_high(attended, out_weight) + out_bias)
    middle = rows + branch
    modulation = matmul_high(time_features(step, TDIM)[None, :], ada_weight)[0] + ada_bias
    shift = modulation[:D]
    scale = modulation[D:2 * D]
    gate = modulation[2 * D:]
    modulated = low(layer_norm(middle) * (1.0 + scale) + shift)
    hidden_pre = low_back(matmul_high(modulated, up_weight) + up_bias)
    hidden = low(jax.nn.gelu(hidden_pre, approximate=True))
    result = low_back(matmul_high(hidden, down_weight) + down_bias)
    return middle + gate * result

def reference(tokens, cotangent, seq_units, deal, timesteps, ln_gain, ln_bias, qkv_weight, qkv_bias, out_weight, out_bias, ada_weight, ada_bias, up_weight, up_bias, down_weight, down_bias):
    params = tuple((w.astype(jnp.float32) for w in (ln_gain, ln_bias, qkv_weight, qkv_bias, out_weight, out_bias, ada_weight, ada_bias, up_weight, up_bias, down_weight, down_bias)))
    starts = (jnp.cumsum(seq_units, axis=1) - seq_units).astype(jnp.int32)
    unit_ids = jnp.arange(UNITS, dtype=jnp.int32)
    member = ((unit_ids[None, None, :] >= starts[:, :, None]) & (unit_ids[None, None, :] < (starts + seq_units)[:, :, None])).astype(jnp.int32)
    seq_of = lax.optimization_barrier(jnp.sum(member * unit_ids[None, :, None], axis=1)).astype(jnp.int32)
    place = lax.optimization_barrier(jnp.sum(member * (unit_ids[None, None, :] - starts[:, :, None]), axis=1)).astype(jnp.int32)
    group_ids = jnp.arange(GROUPS, dtype=jnp.int32)[:, None]

    def forward(inputs, weights):

        def one_group(item):
            group_rows, counts, firsts, steps = item

            def one_sequence(sub):
                count, first, step = sub
                picks = jnp.minimum(first + jnp.arange(2, dtype=jnp.int32), UNITS - 1).astype(jnp.int32)
                rows = group_rows[picks].reshape(2 * TOK_DEV, D)
                return sequence_forward(weights, rows, count, step)
            return lax.map(jax.checkpoint(one_sequence), (counts, firsts, steps))
        outs = lax.map(one_group, (inputs, seq_units, starts, timesteps))
        blocks = outs.reshape(GROUPS, UNITS, 2, TOK_DEV, D)
        return (blocks[group_ids, seq_of, place], outs)
    inputs = tokens.astype(jnp.float32)
    mixed, pull_back, outs = jax.vjp(forward, inputs, params, has_aux=True)
    grad_inputs, grad_params = pull_back(cotangent.astype(jnp.float32))
    seq_ids = jnp.broadcast_to(jnp.arange(UNITS, dtype=jnp.int32)[None, :], (GROUPS, UNITS))
    inverse = jnp.zeros((GROUPS, UNITS), jnp.int32).at[group_ids, deal].set(seq_ids)
    picked = outs[group_ids, inverse]
    units_of = seq_units[group_ids, inverse]
    rows_ok = jnp.arange(2 * TOK_DEV, dtype=jnp.int32)[None, None, :] < (units_of * TOK_DEV)[:, :, None]
    held = jnp.where(rows_ok[..., None], picked, jnp.zeros_like(picked))
    return (mixed.astype(jnp.bfloat16), held.astype(jnp.bfloat16), grad_inputs.astype(jnp.bfloat16), grad_params[0], grad_params[1], grad_params[2], grad_params[3], grad_params[4], grad_params[5], grad_params[6], grad_params[7], grad_params[8], grad_params[9], grad_params[10], grad_params[11])
```

```python
import math

import jax
import jax.numpy as jnp
from jax import lax
from jax.experimental import pallas as pl
from jax.experimental.pallas import tpu as pltpu
from jax.sharding import PartitionSpec as P

HEADS = 12


EPSILON = 1e-05
NEGATIVE = -1000000000.0
HIGHEST = lax.Precision.HIGHEST


def normalize(values):
    center = values - jnp.mean(values, axis=-1, keepdims=True)
    spread = jnp.mean(center * center, axis=-1, keepdims=True)
    inverse = lax.rsqrt(spread + EPSILON)
    return (center * inverse, inverse)


def normalize_back(grad, normed, inverse):
    return inverse * (
        grad
        - jnp.mean(grad, axis=-1, keepdims=True)
        - normed * jnp.mean(grad * normed, axis=-1, keepdims=True)
    )


def rotary_tables(length, head_dim):
    half = head_dim // 2
    freqs = jnp.exp(-math.log(10000.0) * jnp.arange(half, dtype=jnp.float32) / half)
    angles = jnp.arange(length, dtype=jnp.float32)[:, None] * freqs[None, :]
    return (jnp.cos(angles)[:, None, :], jnp.sin(angles)[:, None, :])


def rotate(field, cosines, sines):
    half = field.shape[-1] // 2
    first = field[..., :half]
    second = field[..., half:]
    return jnp.concatenate(
        [first * cosines - second * sines, second * cosines + first * sines], axis=-1
    )


def unrotate(grad, cosines, sines):
    half = grad.shape[-1] // 2
    first = grad[..., :half]
    second = grad[..., half:]
    return jnp.concatenate(
        [first * cosines + second * sines, second * cosines - first * sines], axis=-1
    )


def time_features(step, width):
    half = width // 2
    freqs = jnp.exp(-math.log(10000.0) * jnp.arange(half, dtype=jnp.float32) / half)
    angles = step.astype(jnp.float32) * freqs
    return jnp.concatenate([jnp.cos(angles), jnp.sin(angles)])


def inner_rows(left, right):
    return lax.dot_general(
        left, right, (((0,), (0,)), ((), ())), preferred_element_type=jnp.float32
    )


def times_transposed(left, right):
    return lax.dot_general(
        left, right, (((1,), (1,)), ((), ())), preferred_element_type=jnp.float32
    )


def on_device(
    tokens,
    cotangent,
    seq_units,
    deal,
    timesteps,
    ln_gain,
    ln_bias,
    qkv_weight,
    qkv_bias,
    out_weight,
    out_bias,
    ada_weight,
    ada_bias,
    up_weight,
    up_bias,
    down_weight,
    down_bias,
):
    owners = lax.axis_size("shard")
    myself = lax.axis_index("shard")
    unit_count = tokens.shape[1]
    piece_rows = tokens.shape[2]
    width = tokens.shape[3]
    length = 2 * owners * piece_rows
    block_rows = min(512, length)
    head_count = HEADS
    head_dim = width // head_count
    factor = 1.0 / math.sqrt(head_dim)
    units = seq_units[0]
    dealt = deal[0]
    step_list = timesteps[0]
    starts = jnp.cumsum(units) - units
    unit_ids = jnp.arange(unit_count, dtype=jnp.int32)
    member = (
        (unit_ids[None, :] >= starts[:, None]) & (unit_ids[None, :] < (starts + units)[:, None])
    ).astype(jnp.int32)
    target = jnp.sum(member * dealt[:, None], axis=0)
    place = jnp.sum(member * (unit_ids[None, :] - starts[:, None]), axis=0)
    select = (
        (place[None, None, :] == jnp.arange(2, dtype=jnp.int32)[:, None, None])
        & (target[None, None, :] == jnp.arange(owners, dtype=jnp.int32)[None, :, None])
    ).astype(jnp.bfloat16)
    owned = (dealt == myself) & (units > 0)
    own_units = jnp.sum(jnp.where(owned, units, 0))
    own_step = jnp.sum(jnp.where(owned, step_list, 0))
    key_live = jnp.arange(length, dtype=jnp.int32) < own_units * (owners * piece_rows)

    def deal_rows(local):
        return jnp.einsum(
            "pqk,ktd->pqtd", select, local, preferred_element_type=jnp.float32
        ).astype(jnp.bfloat16)

    def collect_rows(arrived):
        return jnp.einsum(
            "pqk,pqtd->ktd", select, arrived, preferred_element_type=jnp.float32
        ).astype(jnp.bfloat16)[None]

    arrived_rows = lax.all_to_all(
        deal_rows(tokens[0]), "shard", split_axis=1, concat_axis=1, tiled=True
    )
    rows = arrived_rows.reshape(length, width).astype(jnp.float32)
    (
        gain,
        norm_shift,
        qkv_full,
        qkv_add,
        out_full,
        out_add,
        ada_full,
        ada_add,
        up_full,
        up_add,
        down_full,
        down_add,
    ) = (
        lax.all_gather(ln_gain, "shard", axis=0, tiled=True),
        lax.all_gather(ln_bias, "shard", axis=0, tiled=True),
        lax.all_gather(qkv_weight, "shard", axis=0, tiled=True),
        lax.all_gather(qkv_bias, "shard", axis=0, tiled=True),
        lax.all_gather(out_weight, "shard", axis=0, tiled=True),
        lax.all_gather(out_bias, "shard", axis=0, tiled=True),
        lax.all_gather(ada_weight, "shard", axis=0, tiled=True),
        lax.all_gather(ada_bias, "shard", axis=0, tiled=True),
        lax.all_gather(up_weight, "shard", axis=0, tiled=True),
        lax.all_gather(up_bias, "shard", axis=0, tiled=True),
        lax.all_gather(down_weight, "shard", axis=0, tiled=True),
        lax.all_gather(down_bias, "shard", axis=0, tiled=True),
    )
    normed_first, inverse_first = normalize(rows)
    normed_in = (normed_first * gain + norm_shift).astype(jnp.bfloat16)
    projected = jnp.dot(normed_in, qkv_full, preferred_element_type=jnp.float32) + qkv_add
    cosines, sines = rotary_tables(length, head_dim)
    queries = (
        rotate(projected[:, :width].reshape(length, head_count, head_dim), cosines, sines)
        .astype(jnp.bfloat16)
        .transpose(1, 0, 2)
    )
    key_rows = (
        rotate(
            projected[:, width : 2 * width].reshape(length, head_count, head_dim), cosines, sines
        )
        .astype(jnp.bfloat16)
        .transpose(1, 0, 2)
    )
    value_rows = (
        projected[:, 2 * width :]
        .reshape(length, head_count, head_dim)
        .astype(jnp.bfloat16)
        .transpose(1, 0, 2)
    )

    def attend(items):
        query_head, key_head, value_head = items
        outputs = []
        totals = []
        for offset in range(0, length, block_rows):
            query_block = query_head[offset : offset + block_rows]
            scores = (
                jnp.einsum("qd,kd->qk", query_block, key_head, preferred_element_type=jnp.float32)
                * factor
            )
            scores = jnp.where(key_live[None, :], scores, NEGATIVE)
            highest = jnp.max(scores, axis=1, keepdims=True)
            expon = jnp.exp(scores - highest)
            summed = jnp.sum(expon, axis=1, keepdims=True)
            probs = (expon / summed).astype(jnp.bfloat16)
            outputs.append(jnp.dot(probs, value_head, preferred_element_type=jnp.float32))
            totals.append((highest + jnp.log(summed))[:, 0])
        return (jnp.concatenate(outputs, axis=0), jnp.concatenate(totals, axis=0))

    heads_out, log_totals = lax.map(attend, (queries, key_rows, value_rows))
    attended = heads_out.transpose(1, 0, 2).reshape(length, width).astype(jnp.bfloat16)
    middle = rows + jnp.dot(attended, out_full, preferred_element_type=jnp.float32) + out_add
    features = time_features(own_step, ada_full.shape[0])
    modulation = (
        jnp.dot(
            features[None, :],
            ada_full.astype(jnp.float32),
            precision=HIGHEST,
            preferred_element_type=jnp.float32,
        )[0]
        + ada_add
    )
    shift = modulation[:width]
    scale = modulation[width : 2 * width]
    gate = modulation[2 * width :]
    normed_second, inverse_second = normalize(middle)
    modulated = (normed_second * (1.0 + scale) + shift).astype(jnp.bfloat16)
    hidden_pre = jnp.dot(modulated, up_full, preferred_element_type=jnp.float32) + up_add
    hidden = jax.nn.gelu(hidden_pre).astype(jnp.bfloat16)
    result = jnp.dot(hidden, down_full, preferred_element_type=jnp.float32) + down_add
    output_rows = (middle + gate * result).astype(jnp.bfloat16)
    held = jnp.where(key_live[:, None], output_rows, jnp.zeros_like(output_rows))[None, None]
    mixed = collect_rows(
        lax.all_to_all(
            output_rows.reshape(2, owners, piece_rows, width),
            "shard",
            split_axis=1,
            concat_axis=1,
            tiled=True,
        )
    )
    grad_out = (
        lax.all_to_all(deal_rows(cotangent[0]), "shard", split_axis=1, concat_axis=1, tiled=True)
        .reshape(length, width)
        .astype(jnp.float32)
    )
    gain_back, qkv_back, out_back, up_back, down_back = (
        gain,
        qkv_full,
        out_full,
        up_full,
        down_full,
    )
    grad_gate = jnp.sum(grad_out * result, axis=0)
    grad_result = (gate * grad_out).astype(jnp.bfloat16)
    grad_down_bias = jnp.sum(grad_result, axis=0, dtype=jnp.float32)
    grad_down_weight = inner_rows(hidden, grad_result)
    grad_hidden = times_transposed(grad_result, down_back)
    gelu_value, gelu_pull = jax.vjp(jax.nn.gelu, hidden_pre)
    grad_pre = gelu_pull(grad_hidden)[0].astype(jnp.bfloat16)
    grad_up_bias = jnp.sum(grad_pre, axis=0, dtype=jnp.float32)
    grad_up_weight = inner_rows(modulated, grad_pre)
    grad_modulated = times_transposed(grad_pre, up_back)
    grad_scale = jnp.sum(grad_modulated * normed_second, axis=0)
    grad_shift = jnp.sum(grad_modulated, axis=0)
    grad_middle = grad_out + normalize_back(
        grad_modulated * (1.0 + scale), normed_second, inverse_second
    )
    grad_modulation = jnp.concatenate([grad_shift, grad_scale, grad_gate])
    grad_ada_weight = features[:, None] * grad_modulation[None, :]
    grad_branch = grad_middle.astype(jnp.bfloat16)
    grad_out_bias = jnp.sum(grad_branch, axis=0, dtype=jnp.float32)
    grad_out_weight = inner_rows(attended, grad_branch)
    grad_attended = (
        times_transposed(grad_branch, out_back)
        .astype(jnp.bfloat16)
        .reshape(length, head_count, head_dim)
        .transpose(1, 0, 2)
    )

    def attend_back(items):
        query_head, key_head, value_head, grad_head, total_head = items
        grad_keys = jnp.zeros((length, head_dim), jnp.float32)
        grad_values = jnp.zeros((length, head_dim), jnp.float32)
        grad_queries = []
        for offset in range(0, length, block_rows):
            query_block = query_head[offset : offset + block_rows]
            grad_block = grad_head[offset : offset + block_rows]
            scores = (
                jnp.einsum("qd,kd->qk", query_block, key_head, preferred_element_type=jnp.float32)
                * factor
            )
            scores = jnp.where(key_live[None, :], scores, NEGATIVE)
            probs = jnp.exp(scores - total_head[offset : offset + block_rows][:, None])
            probs_low = probs.astype(jnp.bfloat16)
            grad_probs = jnp.einsum(
                "qd,kd->qk", grad_block, value_head, preferred_element_type=jnp.float32
            )
            row_terms = jnp.sum(probs * grad_probs, axis=1, keepdims=True)
            grad_scores = (probs * (grad_probs - row_terms)).astype(jnp.bfloat16)
            grad_values = grad_values + jnp.einsum(
                "qk,qd->kd", probs_low, grad_block, preferred_element_type=jnp.float32
            )
            grad_queries.append(
                jnp.dot(grad_scores, key_head, preferred_element_type=jnp.float32) * factor
            )
            grad_keys = (
                grad_keys
                + jnp.einsum(
                    "qk,qd->kd", grad_scores, query_block, preferred_element_type=jnp.float32
                )
                * factor
            )
        return (jnp.concatenate(grad_queries, axis=0), grad_keys, grad_values)

    grad_queries, grad_keys, grad_values = lax.map(
        attend_back, (queries, key_rows, value_rows, grad_attended, log_totals)
    )
    grad_queries = unrotate(grad_queries.transpose(1, 0, 2), cosines, sines).reshape(length, width)
    grad_keys = unrotate(grad_keys.transpose(1, 0, 2), cosines, sines).reshape(length, width)
    grad_values = grad_values.transpose(1, 0, 2).reshape(length, width)
    grad_projected = jnp.concatenate([grad_queries, grad_keys, grad_values], axis=1).astype(
        jnp.bfloat16
    )
    grad_qkv_bias = jnp.sum(grad_projected, axis=0, dtype=jnp.float32)
    grad_qkv_weight = inner_rows(normed_in, grad_projected)
    grad_normed = times_transposed(grad_projected, qkv_back)
    grad_ln_gain = jnp.sum(grad_normed * normed_first, axis=0)
    grad_ln_bias = jnp.sum(grad_normed, axis=0)
    grad_rows = grad_middle + normalize_back(grad_normed * gain_back, normed_first, inverse_first)
    grad_tokens = collect_rows(
        lax.all_to_all(
            grad_rows.astype(jnp.bfloat16).reshape(2, owners, piece_rows, width),
            "shard",
            split_axis=1,
            concat_axis=1,
            tiled=True,
        )
    )
    (
        owner_gain,
        owner_shift,
        owner_qkv,
        owner_qkv_bias,
        owner_out,
        owner_out_bias,
        owner_ada,
        owner_ada_bias,
        owner_up,
        owner_up_bias,
        owner_down,
        owner_down_bias,
    ) = (
        lax.psum_scatter(
            grad_ln_gain.astype(jnp.bfloat16), "shard", scatter_dimension=0, tiled=True
        ).astype(jnp.float32),
        lax.psum_scatter(
            grad_ln_bias.astype(jnp.bfloat16), "shard", scatter_dimension=0, tiled=True
        ).astype(jnp.float32),
        lax.psum_scatter(
            grad_qkv_weight.astype(jnp.bfloat16), "shard", scatter_dimension=0, tiled=True
        ).astype(jnp.float32),
        lax.psum_scatter(
            grad_qkv_bias.astype(jnp.bfloat16), "shard", scatter_dimension=0, tiled=True
        ).astype(jnp.float32),
        lax.psum_scatter(
            grad_out_weight.astype(jnp.bfloat16), "shard", scatter_dimension=0, tiled=True
        ).astype(jnp.float32),
        lax.psum_scatter(
            grad_out_bias.astype(jnp.bfloat16), "shard", scatter_dimension=0, tiled=True
        ).astype(jnp.float32),
        lax.psum_scatter(
            grad_ada_weight.astype(jnp.bfloat16), "shard", scatter_dimension=0, tiled=True
        ).astype(jnp.float32),
        lax.psum_scatter(
            grad_modulation.astype(jnp.bfloat16), "shard", scatter_dimension=0, tiled=True
        ).astype(jnp.float32),
        lax.psum_scatter(
            grad_up_weight.astype(jnp.bfloat16), "shard", scatter_dimension=0, tiled=True
        ).astype(jnp.float32),
        lax.psum_scatter(
            grad_up_bias.astype(jnp.bfloat16), "shard", scatter_dimension=0, tiled=True
        ).astype(jnp.float32),
        lax.psum_scatter(
            grad_down_weight.astype(jnp.bfloat16), "shard", scatter_dimension=0, tiled=True
        ).astype(jnp.float32),
        lax.psum_scatter(
            grad_down_bias.astype(jnp.bfloat16), "shard", scatter_dimension=0, tiled=True
        ).astype(jnp.float32),
    )
    summed = (
        lax.psum(owner_gain.astype(jnp.bfloat16), "replica").astype(jnp.float32),
        lax.psum(owner_shift.astype(jnp.bfloat16), "replica").astype(jnp.float32),
        lax.psum(owner_qkv.astype(jnp.bfloat16), "replica").astype(jnp.float32),
        lax.psum(owner_qkv_bias.astype(jnp.bfloat16), "replica").astype(jnp.float32),
        lax.psum(owner_out.astype(jnp.bfloat16), "replica").astype(jnp.float32),
        lax.psum(owner_out_bias.astype(jnp.bfloat16), "replica").astype(jnp.float32),
        lax.psum(owner_ada.astype(jnp.bfloat16), "replica").astype(jnp.float32),
        lax.psum(owner_ada_bias.astype(jnp.bfloat16), "replica").astype(jnp.float32),
        lax.psum(owner_up.astype(jnp.bfloat16), "replica").astype(jnp.float32),
        lax.psum(owner_up_bias.astype(jnp.bfloat16), "replica").astype(jnp.float32),
        lax.psum(owner_down.astype(jnp.bfloat16), "replica").astype(jnp.float32),
        lax.psum(owner_down_bias.astype(jnp.bfloat16), "replica").astype(jnp.float32),
    )
    return (mixed, held, grad_tokens) + tuple(summed)


LANES = 128
HEAD_DIM = 64
LOW = jnp.bfloat16
FULL = jnp.float32


def partner(field):
    lane = lax.broadcasted_iota(jnp.int32, field.shape, 1)
    quarter = HEAD_DIM // 2
    return jnp.where(
        lane % HEAD_DIM < quarter,
        pltpu.roll(field, LANES - quarter, 1),
        pltpu.roll(field, quarter, 1),
    )


def one_head(field, head):
    lane = lax.broadcasted_iota(jnp.int32, field.shape, 1)
    return jnp.where(lane // HEAD_DIM == head, field, 0.0).astype(LOW)


def attend_kernel(
    q_ref,
    k_ref,
    v_ref,
    far_k_ref,
    far_v_ref,
    cos_ref,
    sin_ref,
    out_ref,
    q_turned_ref,
    k_turned_ref,
    v_low_ref,
    total_ref,
):
    near = q_ref.shape[0]

    def turn(field, start):
        window = pl.ds(start, near)
        return field * cos_ref[window, :] + partner(field) * sin_ref[window, :]

    queries = turn(q_ref[...], 0).astype(LOW).astype(FULL) * (HEAD_DIM**-0.5)
    q_turned_ref[...] = queries.astype(LOW)
    k_turned_ref[pl.ds(0, near), :] = turn(k_ref[...], 0).astype(LOW)
    k_turned_ref[pl.ds(near, near), :] = turn(far_k_ref[...], near).astype(LOW)
    v_low_ref[pl.ds(0, near), :] = v_ref[...].astype(LOW)
    v_low_ref[pl.ds(near, near), :] = far_v_ref[...].astype(LOW)
    keys = k_turned_ref[...]
    values_across = v_low_ref[...].T
    outs = []
    for head in range(LANES // HEAD_DIM):
        scores = times_transposed(keys, one_head(queries, head))
        highest = jnp.max(scores, axis=0, keepdims=True)
        expon = jnp.exp(scores - highest)
        summed = jnp.sum(expon, axis=0, keepdims=True)
        across = jnp.dot(
            values_across[head * HEAD_DIM : (head + 1) * HEAD_DIM],
            expon.astype(LOW),
            preferred_element_type=FULL,
        )
        outs.append(across / summed)
        total_ref[0, head : head + 1, :] = highest + jnp.log(summed)
    out_ref[...] = jnp.concatenate(outs, axis=0).T.astype(LOW)


def attend(near_rows, far_rows, cosines, sines):
    near = near_rows.shape[0]
    pairs = near_rows.shape[1] // 3 // LANES
    length = 2 * near
    columns = pairs * LANES

    def part(rows, first):
        return pl.BlockSpec((rows, LANES), lambda pair, first=first: (0, first + pair))

    whole = pl.BlockSpec((length, LANES), lambda pair: (0, 0))
    return pl.pallas_call(
        attend_kernel,
        grid=(pairs,),
        in_specs=[
            part(near, 0),
            part(near, pairs),
            part(near, 2 * pairs),
            part(near, 0),
            part(near, pairs),
            whole,
            whole,
        ],
        out_specs=[
            part(near, 0),
            part(near, 0),
            part(length, 0),
            part(length, 0),
            pl.BlockSpec((1, 8, near), lambda pair: (pair, 0, 0)),
        ],
        out_shape=[
            jax.ShapeDtypeStruct((near, columns), LOW),
            jax.ShapeDtypeStruct((near, columns), LOW),
            jax.ShapeDtypeStruct((length, columns), LOW),
            jax.ShapeDtypeStruct((length, columns), LOW),
            jax.ShapeDtypeStruct((pairs, 8, near), FULL),
        ],
        cost_estimate=pl.CostEstimate(
            flops=8 * near * length * columns,
            bytes_accessed=4 * 5 * near * columns + 12 * near * columns,
            transcendentals=near * length * 2 * pairs,
        ),
        name="attend",
    )(near_rows, near_rows, near_rows, far_rows, far_rows, cosines, sines)


def attend_back_kernel(
    q_ref, k_ref, v_ref, grad_ref, total_ref, cos_ref, sin_ref, dq_ref, dk_ref, dv_ref
):
    near = q_ref.shape[0]
    queries = q_ref[...].astype(FULL)
    grads = grad_ref[...].astype(FULL)
    keys = k_ref[...]
    values = v_ref[...]
    keys_across = keys.T
    grad_keys = None
    grad_values = None
    grad_queries = []
    for head in range(LANES // HEAD_DIM):
        query_head = one_head(queries, head)
        grad_head = one_head(grads, head)
        scores = times_transposed(keys, query_head)
        probs = jnp.exp(scores - total_ref[0, head : head + 1, :])
        grad_probs = times_transposed(values, grad_head)
        terms = jnp.sum(probs * grad_probs, axis=0, keepdims=True)
        grad_scores = (probs * (grad_probs - terms)).astype(LOW)
        value_part = jnp.dot(probs.astype(LOW), grad_head, preferred_element_type=FULL)
        key_part = jnp.dot(grad_scores, query_head, preferred_element_type=FULL)
        grad_values = value_part if grad_values is None else grad_values + value_part
        grad_keys = key_part if grad_keys is None else grad_keys + key_part
        grad_queries.append(
            jnp.dot(
                keys_across[head * HEAD_DIM : (head + 1) * HEAD_DIM],
                grad_scores,
                preferred_element_type=FULL,
            )
        )

    def turn_back(field, rows):
        return field * cos_ref[rows, :] - partner(field) * sin_ref[rows, :]

    whole = pl.ds(0, 2 * near)
    dq = jnp.concatenate(grad_queries, axis=0).T * (HEAD_DIM**-0.5)
    dq_ref[...] = turn_back(dq, pl.ds(0, near)).astype(LOW)
    dk_ref[...] = turn_back(grad_keys, whole).astype(LOW)
    dv_ref[...] = grad_values.astype(LOW)


def attend_back(queries, keys, values, grads, totals, cosines, sines):
    near, columns = queries.shape
    pairs = columns // LANES
    length = 2 * near
    row_part = pl.BlockSpec((near, LANES), lambda pair: (0, pair))
    all_part = pl.BlockSpec((length, LANES), lambda pair: (0, pair))
    whole = pl.BlockSpec((length, LANES), lambda pair: (0, 0))
    return pl.pallas_call(
        attend_back_kernel,
        grid=(pairs,),
        in_specs=[
            row_part,
            all_part,
            all_part,
            row_part,
            pl.BlockSpec((1, 8, near), lambda pair: (pair, 0, 0)),
            whole,
            whole,
        ],
        out_specs=[row_part, all_part, all_part],
        out_shape=[
            jax.ShapeDtypeStruct((near, columns), LOW),
            jax.ShapeDtypeStruct((length, columns), LOW),
            jax.ShapeDtypeStruct((length, columns), LOW),
        ],
        cost_estimate=pl.CostEstimate(
            flops=20 * near * length * columns,
            bytes_accessed=2 * 11 * near * columns,
            transcendentals=near * length * 2 * pairs,
        ),
        name="attend_back",
    )(queries, keys, values, grads, totals, cosines, sines)


def swap(array, axis, bit):
    count = lax.axis_size(axis)
    return lax.ppermute(array, axis, [(i, i ^ bit) for i in range(count)])


def pick(array, index, dim=0):
    return lax.dynamic_index_in_dim(array, index, dim, keepdims=False)


def in_order(flag, mine, other, dim=0):
    return jnp.where(
        flag == 0, jnp.stack([mine, other], axis=dim), jnp.stack([other, mine], axis=dim)
    )


def replica_bits():
    index = lax.axis_index("replica")
    levels = lax.axis_size("replica").bit_length() - 1
    return [(1 << level, (index >> level) % 2) for level in range(levels)]


def fetch_other(local):
    (core_bit, core), (side_bit, side) = replica_bits()[:2]
    rows, columns = local.shape
    quarter = pick(local.reshape(4, rows // 4, columns), side * 2 + core)
    quarter = swap(quarter, "shard", 1)
    half = in_order(side, quarter, swap(quarter, "replica", side_bit))
    whole = in_order(core, half, swap(half, "replica", core_bit), 1)
    return whole.reshape(rows, columns)


def gather_rows(local, myself):
    return in_order(myself, local, fetch_other(local)).reshape(
        2 * local.shape[0], local.shape[1]
    )


def halve(blocks, flag, axis, bit, dim=0):
    kept = pick(blocks, flag, dim)
    sent = pick(blocks, 1 - flag, dim)
    return (kept.astype(FULL) + swap(sent, axis, bit).astype(FULL)).astype(LOW)


def reduce_rows(partial, myself):
    columns = partial.shape[1]
    bits = replica_bits()
    part = halve(partial.reshape(2, 2, -1, columns), bits[0][1], "replica", 1, 1)
    part = halve(part, myself, "shard", 1)
    for bit, flag in bits[1:]:
        part = halve(part.reshape(2, -1, columns), flag, "replica", bit)
    for bit, flag in bits[::-1]:
        part = in_order(flag, part, swap(part, "replica", bit)).reshape(-1, columns)
    return part.astype(FULL)


def on_half(
    tokens,
    cotangent,
    seq_units,
    deal,
    timesteps,
    ln_gain,
    ln_bias,
    qkv_weight,
    qkv_bias,
    out_weight,
    out_bias,
    ada_weight,
    ada_bias,
    up_weight,
    up_bias,
    down_weight,
    down_bias,
):
    myself = lax.axis_index("shard")
    unit_count, piece_rows, width = tokens.shape[1:]
    near = unit_count * piece_rows
    used = seq_units[0] > 0
    owner = jnp.sum(jnp.where(used, deal[0], 0))
    own_step = jnp.sum(jnp.where(used, timesteps[0], 0))

    near_tokens = tokens[0].reshape(near, width)
    qkv_full = gather_rows(qkv_weight, myself)
    far_tokens = swap(near_tokens, "shard", 1)
    vectors = (ln_gain, ln_bias, qkv_bias, out_bias, ada_bias, up_bias, down_bias)
    packed = jnp.concatenate(vectors)
    other_packed = swap(packed, "shard", 1)
    gathered = []
    offset = 0
    for vector in vectors:
        size = vector.shape[0]
        gathered.append(
            in_order(myself, vector, other_packed[offset : offset + size])
            .reshape(-1)
            .astype(FULL)
        )
        offset += size
    gain, norm_shift, qkv_add, out_add, ada_add, up_add, down_add = gathered

    ada_rows = ada_weight.shape[0]
    features = time_features(own_step, 2 * ada_rows)
    own_features = pick(features.reshape(2, ada_rows), myself)
    modulation_part = jnp.dot(
        own_features[None, :],
        ada_weight.astype(FULL),
        precision=HIGHEST,
        preferred_element_type=FULL,
    )[0]
    modulation = modulation_part + swap(modulation_part, "shard", 1) + ada_add
    shift = modulation[:width]
    scale = modulation[width : 2 * width]
    gate = modulation[2 * width :]

    half = HEAD_DIM // 2
    lane = jnp.arange(LANES)
    freqs = jnp.exp(-math.log(10000.0) * (lane % half).astype(FULL) / half)
    row = jnp.arange(2 * near)
    holder = jnp.where(row < near, myself, 1 - myself)
    inside = row % near
    position = (inside // piece_rows) * (2 * piece_rows) + holder * piece_rows + inside % piece_rows
    angles = position.astype(FULL)[:, None] * freqs[None, :]
    cosines = jnp.cos(angles)
    sines = jnp.where(lane % HEAD_DIM < half, -1.0, 1.0)[None, :] * jnp.sin(angles)

    rows = near_tokens.astype(FULL)
    near_normed, near_inverse = normalize(rows)
    far_normed, far_inverse = normalize(far_tokens.astype(FULL))
    near_in = (near_normed * gain + norm_shift).astype(LOW)
    far_in = (far_normed * gain + norm_shift).astype(LOW)
    near_rows = jnp.dot(near_in, qkv_full, preferred_element_type=FULL) + qkv_add
    far_rows = (
        jnp.dot(far_in, qkv_full[:, width:], preferred_element_type=FULL) + qkv_add[width:]
    )
    attended, queries, key_rows, value_rows, totals = attend(
        near_rows, far_rows, cosines, sines
    )

    up_full = gather_rows(up_weight, myself)
    down_full = gather_rows(down_weight, myself)
    out_full = gather_rows(out_weight, myself)
    middle = rows + jnp.dot(attended, out_full, preferred_element_type=FULL) + out_add
    normed_second, inverse_second = normalize(middle)
    modulated = (normed_second * (1.0 + scale) + shift).astype(LOW)
    hidden_pre = jnp.dot(modulated, up_full, preferred_element_type=FULL) + up_add
    hidden = jax.nn.gelu(hidden_pre).astype(LOW)
    result = jnp.dot(hidden, down_full, preferred_element_type=FULL) + down_add
    output_rows = (middle + gate * result).astype(LOW)
    mixed = output_rows.reshape(1, unit_count, piece_rows, width)
    own_output = output_rows.reshape(unit_count, piece_rows, width)
    other_output = swap(own_output, "shard", 1)
    held = in_order(myself, own_output, other_output, 1).reshape(2 * near, width)
    held = jnp.where(owner == myself, held, jnp.zeros_like(held))[None, None]

    grad_out = cotangent[0].reshape(near, width).astype(FULL)
    grad_gate = jnp.sum(grad_out * result, axis=0)
    grad_result = (gate * grad_out).astype(LOW)
    grad_down_bias = jnp.sum(grad_result, axis=0, dtype=FULL)
    grad_down_weight = inner_rows(hidden, grad_result).astype(LOW)
    down_sum = reduce_rows(grad_down_weight, myself)
    grad_hidden = times_transposed(grad_result, down_full)
    gelu_pull = jax.vjp(jax.nn.gelu, hidden_pre)[1]
    grad_pre = gelu_pull(grad_hidden)[0].astype(LOW)
    grad_up_bias = jnp.sum(grad_pre, axis=0, dtype=FULL)
    grad_up_weight = inner_rows(modulated, grad_pre).astype(LOW)
    up_sum = reduce_rows(grad_up_weight, myself)
    grad_modulated = times_transposed(grad_pre, up_full)
    grad_scale = jnp.sum(grad_modulated * normed_second, axis=0)
    grad_shift = jnp.sum(grad_modulated, axis=0)
    grad_middle = grad_out + normalize_back(
        grad_modulated * (1.0 + scale), normed_second, inverse_second
    )
    grad_branch = grad_middle.astype(LOW)
    grad_out_bias = jnp.sum(grad_branch, axis=0, dtype=FULL)
    grad_out_weight = inner_rows(attended, grad_branch).astype(LOW)
    out_sum = reduce_rows(grad_out_weight, myself)
    grad_attended = times_transposed(grad_branch, out_full).astype(LOW)

    grad_modulation = jnp.concatenate([grad_shift, grad_scale, grad_gate])
    note = jnp.concatenate([grad_modulation, jnp.full((LANES,), own_step.astype(FULL))])
    notes = lax.all_gather(note, ("replica", "shard"), axis=0)
    all_features = jax.vmap(lambda step: time_features(step, 2 * ada_rows))(
        notes[:, 3 * width]
    )
    kept_features = pick(all_features.reshape(-1, 2, ada_rows), myself, 1)
    all_modulation = notes[:, : 3 * width]
    ada_sum = lax.dot_general(
        kept_features,
        all_modulation,
        (((0,), (0,)), ((), ())),
        precision=HIGHEST,
        preferred_element_type=FULL,
    )
    ada_bias_sum = pick(jnp.sum(all_modulation, axis=0).reshape(2, -1), myself)
    early = lax.psum(
        jnp.concatenate([grad_down_bias, grad_up_bias, grad_out_bias]), ("replica", "shard")
    )
    hidden_units = grad_up_bias.shape[0]
    down_bias_sum = pick(early[:width].reshape(2, -1), myself)
    up_bias_sum = pick(early[width : width + hidden_units].reshape(2, -1), myself)
    out_bias_sum = pick(early[width + hidden_units :].reshape(2, -1), myself)

    grad_queries, grad_keys, grad_values = attend_back(
        queries, key_rows, value_rows, grad_attended, totals, cosines, sines
    )
    both_in = jnp.concatenate([near_in, far_in], axis=0)
    grad_qkv_weight = jnp.concatenate(
        [
            inner_rows(near_in, grad_queries).astype(LOW),
            inner_rows(both_in, grad_keys).astype(LOW),
            inner_rows(both_in, grad_values).astype(LOW),
        ],
        axis=1,
    )
    qkv_sum = reduce_rows(grad_qkv_weight, myself)
    grad_qkv_bias = jnp.concatenate(
        [jnp.sum(g, axis=0, dtype=FULL) for g in (grad_queries, grad_keys, grad_values)]
    )
    from_values = times_transposed(grad_values, qkv_full[:, 2 * width :])
    from_keys = times_transposed(grad_keys, qkv_full[:, width : 2 * width])
    from_queries = times_transposed(grad_queries, qkv_full[:, :width])
    far_grad = from_values[near:] + from_keys[near:]
    near_grad = from_values[:near] + from_keys[:near] + from_queries
    far_back = normalize_back(far_grad * gain, far_normed, far_inverse).astype(LOW)
    near_back = grad_middle + normalize_back(near_grad * gain, near_normed, near_inverse)
    grad_rows = near_back + swap(far_back, "shard", 1).astype(FULL)
    grad_tokens = grad_rows.astype(LOW).reshape(1, unit_count, piece_rows, width)
    grad_ln_gain = jnp.sum(near_grad * near_normed, axis=0) + jnp.sum(
        far_grad * far_normed, axis=0
    )
    grad_ln_bias = jnp.sum(near_grad, axis=0) + jnp.sum(far_grad, axis=0)
    late = lax.psum(
        jnp.concatenate([grad_ln_gain, grad_ln_bias, grad_qkv_bias]), ("replica", "shard")
    )
    gain_sum = pick(late[:width].reshape(2, -1), myself)
    bias_sum = pick(late[width : 2 * width].reshape(2, -1), myself)
    qkv_bias_sum = pick(late[2 * width :].reshape(2, -1), myself)
    return (
        mixed,
        held,
        grad_tokens,
        gain_sum,
        bias_sum,
        qkv_sum,
        qkv_bias_sum,
        out_sum,
        out_bias_sum,
        ada_sum,
        ada_bias_sum,
        up_sum,
        up_bias_sum,
        down_sum,
        down_bias_sum,
    )


def solution(mesh):
    placed = (
        P("replica", None, "shard", None),
        P("replica", None, "shard", None),
        P("replica", None),
        P("replica", None),
        P("replica", None),
        P("shard"),
        P("shard"),
        P("shard", None),
        P("shard"),
        P("shard", None),
        P("shard"),
        P("shard", None),
        P("shard"),
        P("shard", None),
        P("shard"),
        P("shard", None),
        P("shard"),
    )
    halves = mesh.shape["shard"] == 2 and mesh.shape["replica"] in (4, 8, 16, 32)
    return jax.shard_map(
        on_half if halves else on_device,
        mesh=mesh,
        in_specs=placed,
        out_specs=(
            P("replica", None, "shard", None),
            P("replica", "shard", None, None),
            P("replica", None, "shard", None),
            P("shard"),
            P("shard"),
            P("shard", None),
            P("shard"),
            P("shard", None),
            P("shard"),
            P("shard", None),
            P("shard"),
            P("shard", None),
            P("shard"),
            P("shard", None),
            P("shard"),
        ),
        check_vma=False,
    )
```
